256 devices in a mesh: dom: 64 (over x_lo, z, y), orb: 4 (over x_hi, core).
Axes of the slice: x: 4 (x_hi: 2, x_lo: 2; x = x_hi * 2 + x_lo), y: 4, z: 8, core: 2. Of those that a mesh axis runs over, the one named last changes fastest.
Arguments:
- orbitals: bfloat16 [128, 4, 1024, 512], P('dom', None, None, 'orb'), may hold values from -6 to 6
- slot_ids: int32 [128, 4], P('dom'), may hold values from 0 to 15, as said below
- slot_count: int32 [128], P('dom'), may hold values from 1 to 4, as said below
- band_tiles: bfloat16 [16, 3, 512, 512], P(None, None, 'dom', 'orb'), may hold values from -0.15625 to 0.15625
- pattern: int32 [16, 3], replicated, may hold values 0 or 1
- occupation: float32 [16, 512], P(None, 'orb'), may hold values from 0.0005 to 0.005
Outputs:
- rotated: bfloat16 [128, 4, 1024, 512], P('dom', None, None, 'orb')
- density: float32 [128, 1024], P('dom')
The draws below stay inside these ranges and needn't reach their ends.
Inputs may be any that keep to these rules, and one draw needn't show every extreme that they name: `slot_ids`: each row names 4 consecutive orbital blocks counted modulo 16: slot l holds (s + l) mod 16, where the first block s of a grid block may be any of the 16 blocks. The slots in use on grid block g are its first slot_count[g]; some grid block uses all 4.
All inputs are finite; a program needn't handle non-finite values.
Results may differ from the reference program's by a relative error of at most 0.00094.
Values may be sent and summed in bfloat16 or wider, within the bound.
No kernel may reach another device: no remote copies, remote signals or barrier semaphores. Data moves between devices by JAX's collectives and lax.ppermute only.
A program may use at most 128 MiB of HBM per device.

```python
import math
import jax
import jax.numpy as jnp
from jax import lax

NB = 16
OB = 512
BAND = 3
L = 4
P_SIZE = 1024
G = 128


def draw_slot_ids(key, part):
    lowest = jax.random.randint(jax.random.fold_in(key, 11), (G,), 0, NB, dtype=jnp.int32)
    return ((lowest[:, None] + jnp.arange(L, dtype=jnp.int32)[None, :]) % NB).astype(jnp.int32)


def draw_slot_count(key, part):
    first_draw = jax.random.randint(jax.random.fold_in(key, 21), (G,), 0, L, dtype=jnp.int32)
    second = jax.random.randint(jax.random.fold_in(key, 22), (G,), 0, 2, dtype=jnp.int32)
    in_use = 1 + first_draw * second
    return jnp.where(jnp.arange(G, dtype=jnp.int32) == 0, L, in_use).astype(jnp.int32)


def touch_ends(drawn, key, least, largest):
    longest = drawn.shape.index(max(drawn.shape))
    spots = []
    for shift in (0, 1):
        where = [jax.random.randint(jax.random.fold_in(key, axis), (), 0, length) for axis, length in enumerate(drawn.shape)]
        where[longest] = (where[longest] + shift) % drawn.shape[longest]
        spots.append(tuple(where))
    return drawn.at[spots[0]].set(least).at[spots[1]].set(largest)


def shard_levels(key, dims, pieces, least, top_value):
    loudness = 1.0
    for position, parts in pieces:
        draws = jax.random.uniform(jax.random.fold_in(jax.random.fold_in(key, 6), position), (parts,), jnp.float32, least / len(pieces), top_value / len(pieces))
        loudness = loudness * jnp.repeat(jnp.exp(draws), dims[position] // parts).reshape((-1,) + (1,) * (len(dims) - 1 - position))
    return loudness


def normal_values(stream_key, dims, deviation, reach, pieces=(), kind=jnp.bfloat16):
    values = deviation * jax.random.normal(stream_key, dims, jnp.float32)
    if pieces:
        values = values * shard_levels(stream_key, dims, pieces, -0.22, 0.18)
    return jnp.clip(values, -reach, reach).astype(kind)


def setup_inputs(seed: int = 0) -> dict:
    key_list = jax.random.split(jax.random.key(seed), 7)
    return {
        "orbitals": normal_values(key_list[0], (G, L, P_SIZE, OB), 1.0, 6.0, ((0, 64), (3, 4))),
        "slot_ids": draw_slot_ids(jax.random.fold_in(key_list[6], 71), 0),
        "slot_count": draw_slot_count(jax.random.fold_in(key_list[6], 71), 0),
        "band_tiles": normal_values(key_list[3], (NB, BAND, OB, OB), (OB * BAND) ** -0.5, 0.15625, ((2, 64), (3, 4))),
        "pattern": touch_ends((jax.random.randint(key_list[4], (NB, BAND), 0, 4) < 3).astype(jnp.int32), jax.random.fold_in(key_list[4], 1), 0, 1),
        "occupation": jnp.clip(jnp.exp(math.log(0.005) - 2.30258502 * jax.random.uniform(key_list[5], (NB, OB), jnp.float32) ** shard_levels(key_list[5], (NB, OB), ((1, 4),), -0.2, 0.2)), 0.0005, 0.005),
    }


def select_tiles(band_tiles, pattern, block_ids, block_count):
    slots_per = block_ids.shape[0]
    band_count = pattern.shape[1]
    half_band = (band_count - 1) // 2
    active = jnp.arange(slots_per, dtype=jnp.int32) < block_count
    source = block_ids[:, None]
    target = block_ids[None, :]
    offset = target - source + half_band
    inside = (offset >= 0) & (offset < band_count)
    column = jnp.clip(offset, 0, band_count - 1).astype(jnp.int32)
    keeping = inside & (pattern[source, column] == 1) & active[:, None] & active[None, :]
    picked = band_tiles[source, column]
    return jnp.where(keeping[:, :, None, None], picked, jnp.zeros((), picked.dtype))


def reference(orbitals, slot_ids, slot_count, band_tiles, pattern, occupation):
    def one_block(block_items):
        values, block_ids, block_count = block_items
        tile_set = select_tiles(band_tiles, pattern, block_ids, block_count)
        rotated = jnp.einsum('lpi,lmij->mpj', values.astype(jnp.float32), tile_set.astype(jnp.float32), precision=lax.Precision.HIGHEST).astype(jnp.bfloat16)
        weights = occupation[block_ids]
        square = rotated.astype(jnp.float32) * rotated.astype(jnp.float32)
        density = jnp.einsum('mpj,mj->p', square, weights, precision=lax.Precision.HIGHEST)
        return rotated, density

    rotated, density = lax.map(one_block, (orbitals, slot_ids, slot_count))
    return (rotated, density)
```

```python
import jax
import jax.numpy as jnp
from jax import lax
from jax.experimental import pallas as pl
from jax.experimental.pallas import tpu as pltpu
from jax.sharding import Mesh
from jax.sharding import PartitionSpec as P


DOM = ("xl", "z", "y")
ORB = ("xh", "c")

NEAR = (1, 3, 7, 2)
FAR = (6, 5, 4)
PEERS = (1, 3, 2)
PAIRS = tuple((l, l) for l in range(4)) + tuple((l, l + 1) for l in range(3)) + tuple((l + 1, l) for l in range(3))
CHUNK = 256


def swap(x, axis, distance=1):
    size = lax.axis_size(axis)
    return lax.ppermute(x, axis, [(i, i ^ distance) for i in range(size)])


def pack_kernel(*refs):
    peers = len(PEERS)
    ids, pieces, outs = refs[:peers], refs[peers:-peers], refs[-peers:]
    for g in range(2):
        for n, (source, target) in enumerate(PAIRS):
            for slots, out in zip(ids, outs):
                tile = slots[g, source] * 3 + (target - source + 1)
                for k, piece in enumerate(pieces):
                    for half in range(2):
                        out[g * len(PAIRS) + n, k, half] = piece[half, tile]


def pack(slots, pieces):
    shape = jax.ShapeDtypeStruct((2 * len(PAIRS), len(pieces), *pieces[0].shape[:1], *pieces[0].shape[2:]), pieces[0].dtype)
    smem = pl.BlockSpec(memory_space=pltpu.SMEM)
    vmem = pl.BlockSpec(memory_space=pltpu.VMEM)
    return pl.pallas_call(
        pack_kernel,
        out_shape=[shape] * len(slots),
        in_specs=[smem] * len(slots) + [vmem] * len(pieces),
        out_specs=[vmem] * len(slots),
        cost_estimate=pl.CostEstimate(flops=1000000, bytes_accessed=2000000, transcendentals=0),
    )(*slots, *pieces)


def rotate_kernel(meta, slots, counts, pattern, *refs):
    own = refs[: 1 + len(NEAR) + len(FAR)]
    rest = refs[len(own) :]
    first, rest = rest[: len(PEERS)], rest[len(PEERS) :]
    second, rest = rest[: len(PEERS)], rest[len(PEERS) :]
    occupation, quarters, (out, density), (weights,) = rest[0], rest[1:5], rest[5:7], rest[7:]
    g = pl.program_id(0)
    my_xl, my_z, my_y, my_q = meta[0], meta[1], meta[2], meta[3]
    distances = (0,) + NEAR + FAR
    pairs = len(PAIRS)

    @pl.when(pl.program_id(1) == 0)
    def _():
        zero = jnp.zeros((8, 128), weights.dtype)
        weights[0, 2, :, :, :, :, :128] = jnp.zeros((4, 4, 4, 8, 128), weights.dtype)
        weights[1, 0, :, :, :, :, 128:] = jnp.zeros((4, 4, 4, 8, 128), weights.dtype)
        for n, (source, target) in enumerate(PAIRS):
            s, t = slots[g, source], slots[g, target]
            column = target - source + 1
            keep = (t - s == target - source) & (pattern[s, column] == 1) & (max(source, target) < counts[g])
            tile = s * 3 + column
            pair = target // 2
            row = source - pair
            lanes = slice(128 * (target % 2), 128 * (target % 2) + 128)
            for k, distance in enumerate(distances):
                z = my_z ^ distance
                for half in range(2):
                    quarter = ((my_xl ^ half) * 2 + z // 4) ^ my_q
                    for y in (0,) + PEERS:
                        if y == 0:
                            block = own[k][half, tile]
                        elif k <= len(NEAR):
                            block = first[PEERS.index(y)][g * pairs + n, k, half]
                        else:
                            block = second[PEERS.index(y)][g * pairs + n, k - 1 - len(NEAR), half]
                        weights[pair, row, quarter, z % 4, my_y ^ y, :, lanes] = jnp.where(keep, block, zero)

    total = jnp.zeros((CHUNK, 128), jnp.float32)
    left = [jnp.concatenate([q[0, l] for q in quarters], axis=1) for l in range(4)]
    for pair in range(2):
        acc = None
        for row in range(3):
            w = weights[pair, row].reshape(512, 256)
            part = jnp.dot(left[row + pair], w, preferred_element_type=jnp.float32)
            acc = part if acc is None else acc + part
        rounded = acc.astype(out.dtype)
        for m in range(2):
            mine = rounded[:, 128 * m : 128 * m + 128]
            out[0, 2 * pair + m] = mine
            wide = mine.astype(jnp.float32)
            total = total + wide * wide * occupation[pl.ds(slots[g, 2 * pair + m], 1), :]
    density[0] = lax.dot_general(
        jnp.ones((8, 128), jnp.float32), total, (((1,), (1,)), ((), ())),
        precision=lax.Precision.HIGHEST, preferred_element_type=jnp.float32,
    )[:1]


def rotate(meta, slot_ids, slot_count, pattern, own, first, second, occupation, quarters):
    blocks, slots_per, points, width = quarters[0].shape
    smem = pl.BlockSpec(memory_space=pltpu.SMEM)
    vmem = pl.BlockSpec(memory_space=pltpu.VMEM)
    tile = pl.BlockSpec((1, slots_per, CHUNK, width), lambda g, p: (g, 0, p, 0))
    return pl.pallas_call(
        rotate_kernel,
        grid=(blocks, points // CHUNK),
        out_shape=[
            jax.ShapeDtypeStruct(quarters[0].shape, quarters[0].dtype),
            jax.ShapeDtypeStruct((blocks, 1, points), jnp.float32),
        ],
        in_specs=[smem] * 4 + [vmem] * (len(own) + len(first) + len(second) + 1) + [tile] * 4,
        out_specs=[tile, pl.BlockSpec((1, 1, CHUNK), lambda g, p: (g, 0, p))],
        scratch_shapes=[pltpu.VMEM((2, 3, 4, 4, 4, 8, 256), jnp.bfloat16)],
        compiler_params=pltpu.CompilerParams(dimension_semantics=("arbitrary", "arbitrary")),
        cost_estimate=pl.CostEstimate(flops=3 * 10**9, bytes_accessed=14 * 10**6, transcendentals=0),
    )(meta, slot_ids, slot_count, pattern, *own, *first, *second, occupation, *quarters)


def body(orbitals, slot_ids, slot_count, band_tiles, pattern, occupation):
    rows = band_tiles.shape[2]
    meta = jnp.stack(
        [lax.axis_index("xl"), lax.axis_index("z"), lax.axis_index("y"), lax.axis_index("xh") * 2 + lax.axis_index("c")]
    ).astype(jnp.int32)
    tiles = band_tiles.reshape(-1, rows, band_tiles.shape[3])
    here = jnp.stack([tiles, swap(tiles, "xl")])
    far_half = swap(orbitals, "xh")
    near_half = swap(orbitals, "c")
    slots = [swap(slot_ids, "y", k) for k in PEERS]
    near = [here] + [swap(here, "z", k) for k in NEAR]
    far = [swap(here, "z", k) for k in FAR]
    packed = pack(slots, near)
    first = [swap(x, "y", k) for x, k in zip(packed, PEERS)]
    packed = pack(slots, far)
    second = [swap(x, "y", k) for x, k in zip(packed, PEERS)]
    quarters = [orbitals, near_half, far_half, swap(far_half, "c")]
    rotated, partial = rotate(meta, slot_ids, slot_count, pattern, near + far, first, second, occupation, quarters)
    partial = partial[:, 0]
    chip = partial + swap(partial, "c")
    return rotated, chip + swap(chip, "xh")


def solution(mesh):
    sizes = (2, 8, 4, 2, 2)
    torus = Mesh(mesh.devices.reshape(sizes), DOM + ORB)
    return jax.shard_map(
        body,
        mesh=torus,
        in_specs=(
            P(DOM, None, None, ORB),
            P(DOM, None),
            P(DOM),
            P(None, None, DOM, ORB),
            P(),
            P(None, ORB),
        ),
        out_specs=(P(DOM, None, None, ORB), P(DOM, None)),
        check_vma=False,
    )
```

```python
import jax
import jax.numpy as jnp
from jax import lax
from jax.experimental import pallas as pl
from jax.experimental.pallas import tpu as pltpu
from jax.sharding import Mesh
from jax.sharding import PartitionSpec as P


DOM = ("xl", "z", "y")
ORB = ("xh", "c")

PEERS = (1, 3, 2)
GROUPS = (3, 2, 3)
EARLY, LATE = GROUPS[0] + GROUPS[1], GROUPS[2]
PAIRS = tuple((l, l) for l in range(4)) + tuple((l, l + 1) for l in range(3)) + tuple((l + 1, l) for l in range(3))
CHUNK = 1024
SMEM = pl.BlockSpec(memory_space=pltpu.SMEM)
VMEM = pl.BlockSpec(memory_space=pltpu.VMEM)


def permute(x, axis, target):
    size = lax.axis_size(axis)
    return lax.ppermute(x, axis, [(i, target(i) % size) for i in range(size)])


def swap(x, axis, distance=1):
    return permute(x, axis, lambda i: i ^ distance)


def pack_kernel(*refs):
    peers = len(PEERS)
    ids, pieces, outs = refs[:peers], refs[peers:-peers], refs[-peers:]
    for g in range(2):
        for n, (source, target) in enumerate(PAIRS):
            for slots, out in zip(ids, outs):
                tile = slots[g, source] * 3 + (target - source + 1)
                for k, piece in enumerate(pieces):
                    for half in range(2):
                        out[g * len(PAIRS) + n, k, half] = piece[half, tile]


def pack(slots, pieces):
    shape = jax.ShapeDtypeStruct((2 * len(PAIRS), len(pieces), *pieces[0].shape[:1], *pieces[0].shape[2:]), pieces[0].dtype)
    return pl.pallas_call(
        pack_kernel,
        out_shape=[shape] * len(slots),
        in_specs=[SMEM] * len(slots) + [VMEM] * len(pieces),
        out_specs=[VMEM] * len(slots),
        compiler_params=pltpu.CompilerParams(vmem_limit_bytes=8 * 2**20),
        cost_estimate=pl.CostEstimate(flops=1000000, bytes_accessed=2000000, transcendentals=0),
    )(*slots, *pieces)


def tile_of(n, g, slots, counts, pattern):
    source, target = PAIRS[n]
    s, t = slots[g, source], slots[g, target]
    column = target - source + 1
    keep = (t - s == target - source) & (pattern[s, column] == 1) & (max(source, target) < counts[g])
    pair = target // 2
    return s * 3 + column, keep, (pair, source - pair, slice(128 * (target % 2), 128 * (target % 2) + 128))


def place(weights, lead, spot, keep, meta, k, parts):
    pair, row, lanes = spot
    my_xl, my_y, my_q, z = meta[0], meta[1], meta[2], meta[3 + k]
    low, high = my_y % 2 == 1, my_y // 2 == 1
    for half, blocks in enumerate(parts):
        quarter = ((my_xl ^ half) * 2 + z // 4) ^ my_q
        start = pl.multiple_of(quarter * 128 + (z % 4) * 32, 32)
        b = [jnp.where(low, blocks[j ^ 1], blocks[j]) for j in range(4)]
        b = [jnp.where(high, b[j ^ 2], b[j]) for j in range(4)]
        group = jnp.concatenate(b, axis=0)
        weights[(*lead, pair, row, pl.ds(start, 32), lanes)] = jnp.where(keep, group, jnp.zeros_like(group))


def parts_of(own, recv, tile, index, k):
    by_distance = dict(zip(PEERS, recv))
    return [
        [own[half, tile]] + [by_distance[j][index, k, half] for j in (1, 2, 3)]
        for half in range(2)
    ]


def assemble_kernel(meta, slots, counts, pattern, *refs):
    own, weights = refs[:EARLY], refs[-1]
    recv = (refs[EARLY : EARLY + 3], refs[EARLY + 3 : EARLY + 6])
    for g in range(2):
        weights[g, 0, 2, :, :128] = jnp.zeros((512, 128), weights.dtype)
        weights[g, 1, 0, :, 128:] = jnp.zeros((512, 128), weights.dtype)
        for n in range(len(PAIRS)):
            tile, keep, spot = tile_of(n, g, slots, counts, pattern)
            for k in range(EARLY):
                part = 0 if k < GROUPS[0] else 1
                parts = parts_of(own[k], recv[part], tile, g * len(PAIRS) + n, k - part * GROUPS[0])
                place(weights, (g,), spot, keep, meta, k, parts)


def assemble(meta, slot_ids, slot_count, pattern, own, recv):
    return pl.pallas_call(
        assemble_kernel,
        out_shape=jax.ShapeDtypeStruct((2, 2, 3, 512, 256), jnp.bfloat16),
        in_specs=[SMEM] * 4 + [VMEM] * (len(own) + len(recv)),
        out_specs=VMEM,
        compiler_params=pltpu.CompilerParams(vmem_limit_bytes=12 * 2**20),
        cost_estimate=pl.CostEstimate(flops=1000000, bytes_accessed=6000000, transcendentals=0),
    )(meta, slot_ids, slot_count, pattern, *own, *recv)


def rotate_kernel(meta, slots, counts, pattern, staged, *refs):
    own, recv, occupation, quarters = refs[:LATE], refs[LATE : LATE + 3], refs[LATE + 3], refs[LATE + 4 : LATE + 8]
    out, density, weights = refs[LATE + 8 :]
    g, p = pl.program_id(0), pl.program_id(1)

    @pl.when(p == 0)
    def _():
        for pair in range(2):
            for row in range(3):
                weights[pair, row] = staged[0, pair, row]
        for n in range(len(PAIRS)):
            tile, keep, spot = tile_of(n, g, slots, counts, pattern)
            for k in range(LATE):
                place(weights, (), spot, keep, meta, EARLY + k, parts_of(own[k], recv, tile, g * len(PAIRS) + n, k))

    total = jnp.zeros((CHUNK, 128), jnp.float32)
    left = [jnp.concatenate([q[0, l] for q in quarters], axis=1) for l in range(4)]
    for pair in range(2):
        acc = None
        for row in range(3):
            part = jnp.dot(left[row + pair], weights[pair, row], preferred_element_type=jnp.float32)
            acc = part if acc is None else acc + part
        rounded = acc.astype(out.dtype)
        for m in range(2):
            mine = rounded[:, 128 * m : 128 * m + 128]
            out[0, 2 * pair + m] = mine
            wide = mine.astype(jnp.float32)
            total = total + wide * wide * occupation[pl.ds(slots[g, 2 * pair + m], 1), :]
    summed = lax.dot_general(
        jnp.ones((8, 128), jnp.float32), total, (((1,), (1,)), ((), ())),
        precision=lax.Precision.HIGHEST, preferred_element_type=jnp.float32,
    )[:1]
    density[pl.ds(g, 1), pl.ds(pl.multiple_of(p * CHUNK, CHUNK), CHUNK)] = summed


def rotate(meta, slot_ids, slot_count, pattern, staged, own, recv, occupation, quarters):
    blocks, slots_per, points, width = quarters[0].shape
    tile = pl.BlockSpec((1, slots_per, CHUNK, width), lambda g, p: (g, 0, p, 0))
    return pl.pallas_call(
        rotate_kernel,
        grid=(blocks, points // CHUNK),
        out_shape=[
            jax.ShapeDtypeStruct(quarters[0].shape, quarters[0].dtype),
            jax.ShapeDtypeStruct((blocks, points), jnp.float32),
        ],
        in_specs=[SMEM] * 4
        + [pl.BlockSpec((1, *staged.shape[1:]), lambda g, p: (g, 0, 0, 0, 0))]
        + [VMEM] * (len(own) + len(recv) + 1)
        + [tile] * 4,
        out_specs=[tile, pl.BlockSpec((blocks, points), lambda g, p: (0, 0))],
        scratch_shapes=[pltpu.VMEM(staged.shape[1:], jnp.bfloat16)],
        compiler_params=pltpu.CompilerParams(
            dimension_semantics=("arbitrary", "arbitrary"), vmem_limit_bytes=32 * 2**20
        ),
        cost_estimate=pl.CostEstimate(flops=3 * 10**9, bytes_accessed=14 * 10**6, transcendentals=0),
    )(meta, slot_ids, slot_count, pattern, staged, *own, *recv, occupation, *quarters)


def body(orbitals, slot_ids, slot_count, band_tiles, pattern, occupation):
    rows = band_tiles.shape[2]
    z, y = lax.axis_index("z"), lax.axis_index("y")
    odd, second_bit = z % 2, z // 2 % 2
    step = jnp.where(odd == 1, -1, 1)
    z_of = [z, z + step, z - step, z ^ 2, jnp.where(second_bit == 1, z + 2, z - 2), z + 3 * step, z - 3 * step, z + 4]
    meta = jnp.stack(
        [lax.axis_index("xl"), y, lax.axis_index("xh") * 2 + lax.axis_index("c")] + [k & 7 for k in z_of]
    ).astype(jnp.int32)
    tiles = band_tiles.reshape(-1, rows, band_tiles.shape[3])
    here = jnp.stack([tiles, swap(tiles, "xl")])
    far_half = swap(orbitals, "xh")
    near_half = swap(orbitals, "c")
    slots = [swap(slot_ids, "y", k) for k in PEERS]

    def even(i):
        return i ^ 1

    def uneven(i):
        return ((i - 1) ^ 1) + 1

    one = [permute(here, "z", even), permute(here, "z", uneven)]
    two = [swap(here, "z", 2), permute(here, "z", lambda i: ((i - 2) ^ 2) + 2)]
    flag = odd != second_bit
    three = [permute(jnp.where(flag, two[0], two[1]), "z", even), permute(jnp.where(flag, two[1], two[0]), "z", uneven)]
    groups = [[here, *one], two, [*three, swap(here, "z", 4)]]
    recv = []
    for blocks in groups:
        packed = pack(slots, blocks)
        recv.append([swap(x, "y", k) for x, k in zip(packed, PEERS)])
    quarters = [orbitals, near_half, far_half, swap(far_half, "c")]
    staged = assemble(meta, slot_ids, slot_count, pattern, groups[0] + groups[1], recv[0] + recv[1])
    rotated, partial = rotate(meta, slot_ids, slot_count, pattern, staged, groups[2], recv[2], occupation, quarters)
    across = swap(partial, "xh")
    diagonal = permute(partial, ("xh", "c"), lambda i: i ^ 3)
    beside = swap(partial, "c")
    return rotated, (partial + beside) + (across + diagonal)


def solution(mesh):
    sizes = (2, 8, 4, 2, 2)
    torus = Mesh(mesh.devices.reshape(sizes), DOM + ORB)
    return jax.shard_map(
        body,
        mesh=torus,
        in_specs=(
            P(DOM, None, None, ORB),
            P(DOM, None),
            P(DOM),
            P(None, None, DOM, ORB),
            P(),
            P(None, ORB),
        ),
        out_specs=(P(DOM, None, None, ORB), P(DOM, None)),
        check_vma=False,
    )
```

```python
import jax
import jax.numpy as jnp
from jax import lax
from jax.experimental import pallas as pl
from jax.experimental.pallas import tpu as pltpu
from jax.sharding import Mesh
from jax.sharding import PartitionSpec as P


DOM = ("xl", "z", "y")
ORB = ("xh", "c")

PEERS = (1, 3, 2)
GROUPS = (3, 2, 3)
EARLY, LATE = GROUPS[0] + GROUPS[1], GROUPS[2]
PAIRS = tuple((l, l) for l in range(4)) + tuple((l, l + 1) for l in range(3)) + tuple((l + 1, l) for l in range(3))
CHUNK = 1024
SMEM = pl.BlockSpec(memory_space=pltpu.SMEM)
VMEM = pl.BlockSpec(memory_space=pltpu.VMEM)


def permute(x, axis, target):
    size = lax.axis_size(axis)
    return lax.ppermute(x, axis, [(i, target(i) % size) for i in range(size)])


def swap(x, axis, distance=1):
    return permute(x, axis, lambda i: i ^ distance)


def pack_kernel(*refs):
    peers = len(PEERS)
    ids, pieces, outs = refs[:peers], refs[peers:-peers], refs[-peers:]
    for g in range(2):
        for n, (source, target) in enumerate(PAIRS):
            for slots, out in zip(ids, outs):
                tile = slots[g, source] * 3 + (target - source + 1)
                for k, piece in enumerate(pieces):
                    for half in range(2):
                        out[g * len(PAIRS) + n, k, half] = piece[half, tile]


def pack(slots, pieces):
    shape = jax.ShapeDtypeStruct((2 * len(PAIRS), len(pieces), *pieces[0].shape[:1], *pieces[0].shape[2:]), pieces[0].dtype)
    return pl.pallas_call(
        pack_kernel,
        out_shape=[shape] * len(slots),
        in_specs=[SMEM] * len(slots) + [VMEM] * len(pieces),
        out_specs=[VMEM] * len(slots),
        compiler_params=pltpu.CompilerParams(vmem_limit_bytes=8 * 2**20),
        cost_estimate=pl.CostEstimate(flops=1000000, bytes_accessed=2000000, transcendentals=0),
    )(*slots, *pieces)


def tile_of(n, g, slots, counts, pattern):
    source, target = PAIRS[n]
    s, t = slots[g, source], slots[g, target]
    column = target - source + 1
    keep = (t - s == target - source) & (pattern[s, column] == 1) & (max(source, target) < counts[g])
    pair = target // 2
    return s * 3 + column, keep, (pair, source - pair, slice(128 * (target % 2), 128 * (target % 2) + 128))


def place(weights, lead, spot, keep, meta, k, parts):
    pair, row, lanes = spot
    my_xl, my_y, my_q, z = meta[0], meta[1], meta[2], meta[3 + k]
    low, high = my_y % 2 == 1, my_y // 2 == 1
    for half, blocks in enumerate(parts):
        quarter = ((my_xl ^ half) * 2 + z // 4) ^ my_q
        start = pl.multiple_of(row * 512 + quarter * 128 + (z % 4) * 32, 32)
        b = [jnp.where(low, blocks[j ^ 1], blocks[j]) for j in range(4)]
        b = [jnp.where(high, b[j ^ 2], b[j]) for j in range(4)]
        group = jnp.concatenate(b, axis=0)
        weights[(*lead, pair, pl.ds(start, 32), lanes)] = jnp.where(keep, group, jnp.zeros_like(group))


def parts_of(own, recv, tile, index, k):
    by_distance = dict(zip(PEERS, recv))
    return [
        [own[half, tile]] + [by_distance[j][index, k, half] for j in (1, 2, 3)]
        for half in range(2)
    ]


def assemble_kernel(meta, slots, counts, pattern, *refs):
    own, weights = refs[:EARLY], refs[-1]
    recv = (refs[EARLY : EARLY + 3], refs[EARLY + 3 : EARLY + 6])
    for g in range(2):
        weights[g, 0, 1024:, :128] = jnp.zeros((512, 128), weights.dtype)
        weights[g, 1, :512, 128:] = jnp.zeros((512, 128), weights.dtype)
        for n in range(len(PAIRS)):
            tile, keep, spot = tile_of(n, g, slots, counts, pattern)
            for k in range(EARLY):
                part = 0 if k < GROUPS[0] else 1
                parts = parts_of(own[k], recv[part], tile, g * len(PAIRS) + n, k - part * GROUPS[0])
                place(weights, (g,), spot, keep, meta, k, parts)


def assemble(meta, slot_ids, slot_count, pattern, own, recv):
    return pl.pallas_call(
        assemble_kernel,
        out_shape=jax.ShapeDtypeStruct((2, 2, 1536, 256), jnp.bfloat16),
        in_specs=[SMEM] * 4 + [VMEM] * (len(own) + len(recv)),
        out_specs=VMEM,
        compiler_params=pltpu.CompilerParams(vmem_limit_bytes=12 * 2**20),
        cost_estimate=pl.CostEstimate(flops=1000000, bytes_accessed=6000000, transcendentals=0),
    )(meta, slot_ids, slot_count, pattern, *own, *recv)


def rotate_kernel(meta, slots, counts, pattern, staged, *refs):
    own, recv, occupation, quarters = refs[:LATE], refs[LATE : LATE + 3], refs[LATE + 3], refs[LATE + 4 : LATE + 8]
    out, density, weights = refs[LATE + 8 :]
    g, p = pl.program_id(0), pl.program_id(1)

    @pl.when(p == 0)
    def _():
        for pair in range(2):
            weights[pair] = staged[0, pair]
        for n in range(len(PAIRS)):
            tile, keep, spot = tile_of(n, g, slots, counts, pattern)
            for k in range(LATE):
                place(weights, (), spot, keep, meta, EARLY + k, parts_of(own[k], recv, tile, g * len(PAIRS) + n, k))

    total = jnp.zeros((CHUNK, 128), jnp.float32)
    for pair in range(2):
        left = jnp.concatenate([q[0, pair + row] for row in range(3) for q in quarters], axis=1)
        acc = jnp.dot(left, weights[pair], preferred_element_type=jnp.float32)
        rounded = acc.astype(out.dtype)
        for m in range(2):
            mine = rounded[:, 128 * m : 128 * m + 128]
            out[0, 2 * pair + m] = mine
            wide = mine.astype(jnp.float32)
            total = total + wide * wide * occupation[pl.ds(slots[g, 2 * pair + m], 1), :]
    summed = lax.dot_general(
        jnp.ones((8, 128), jnp.float32), total, (((1,), (1,)), ((), ())),
        precision=lax.Precision.HIGHEST, preferred_element_type=jnp.float32,
    )[:1]
    density[pl.ds(g, 1), pl.ds(pl.multiple_of(p * CHUNK, CHUNK), CHUNK)] = summed


def rotate(meta, slot_ids, slot_count, pattern, staged, own, recv, occupation, quarters):
    blocks, slots_per, points, width = quarters[0].shape
    tile = pl.BlockSpec((1, slots_per, CHUNK, width), lambda g, p: (g, 0, p, 0))
    return pl.pallas_call(
        rotate_kernel,
        grid=(blocks, points // CHUNK),
        out_shape=[
            jax.ShapeDtypeStruct(quarters[0].shape, quarters[0].dtype),
            jax.ShapeDtypeStruct((blocks, points), jnp.float32),
        ],
        in_specs=[SMEM] * 4
        + [pl.BlockSpec((1, *staged.shape[1:]), lambda g, p: (g, 0, 0, 0))]
        + [VMEM] * (len(own) + len(recv) + 1)
        + [tile] * 4,
        out_specs=[tile, pl.BlockSpec((blocks, points), lambda g, p: (0, 0))],
        scratch_shapes=[pltpu.VMEM(staged.shape[1:], jnp.bfloat16)],
        compiler_params=pltpu.CompilerParams(
            dimension_semantics=("arbitrary", "arbitrary"), vmem_limit_bytes=32 * 2**20
        ),
        cost_estimate=pl.CostEstimate(flops=3 * 10**9, bytes_accessed=14 * 10**6, transcendentals=0),
    )(meta, slot_ids, slot_count, pattern, staged, *own, *recv, occupation, *quarters)


def body(orbitals, slot_ids, slot_count, band_tiles, pattern, occupation):
    rows = band_tiles.shape[2]
    z, y = lax.axis_index("z"), lax.axis_index("y")
    odd, second_bit = z % 2, z // 2 % 2
    step = jnp.where(odd == 1, -1, 1)
    z_of = [z, z + step, z - step, z ^ 2, jnp.where(second_bit == 1, z + 2, z - 2), z + 3 * step, z - 3 * step, z + 4]
    meta = jnp.stack(
        [lax.axis_index("xl"), y, lax.axis_index("xh") * 2 + lax.axis_index("c")] + [k & 7 for k in z_of]
    ).astype(jnp.int32)
    tiles = band_tiles.reshape(-1, rows, band_tiles.shape[3])
    here = jnp.stack([tiles, swap(tiles, "xl")])
    far_half = swap(orbitals, "xh")
    near_half = swap(orbitals, "c")
    slots = [swap(slot_ids, "y", k) for k in PEERS]

    def even(i):
        return i ^ 1

    def uneven(i):
        return ((i - 1) ^ 1) + 1

    one = [permute(here, "z", even), permute(here, "z", uneven)]
    two = [swap(here, "z", 2), permute(here, "z", lambda i: ((i - 2) ^ 2) + 2)]
    flag = odd != second_bit
    three = [permute(jnp.where(flag, two[0], two[1]), "z", even), permute(jnp.where(flag, two[1], two[0]), "z", uneven)]
    groups = [[here, *one], two, [*three, swap(two[1], "z", 2)]]
    recv = []
    for blocks in groups:
        packed = pack(slots, blocks)
        recv.append([swap(x, "y", k) for x, k in zip(packed, PEERS)])
    quarters = [orbitals, near_half, far_half, swap(far_half, "c")]
    staged = assemble(meta, slot_ids, slot_count, pattern, groups[0] + groups[1], recv[0] + recv[1])
    rotated, partial = rotate(meta, slot_ids, slot_count, pattern, staged, groups[2], recv[2], occupation, quarters)
    across = swap(partial, "xh")
    diagonal = permute(partial, ("xh", "c"), lambda i: i ^ 3)
    beside = swap(partial, "c")
    return rotated, (partial + beside) + (across + diagonal)


def solution(mesh):
    sizes = (2, 8, 4, 2, 2)
    torus = Mesh(mesh.devices.reshape(sizes), DOM + ORB)
    return jax.shard_map(
        body,
        mesh=torus,
        in_specs=(
            P(DOM, None, None, ORB),
            P(DOM, None),
            P(DOM),
            P(None, None, DOM, ORB),
            P(),
            P(None, ORB),
        ),
        out_specs=(P(DOM, None, None, ORB), P(DOM, None)),
        check_vma=False,
    )
```

```python
import jax
import jax.numpy as jnp
from jax import lax
from jax.experimental import pallas as pl
from jax.experimental.pallas import tpu as pltpu
from jax.sharding import Mesh
from jax.sharding import PartitionSpec as P


DOM = ("xl", "z", "y")
ORB = ("xh", "c")

PEERS = (2, 1, 3)
GROUPS = (3, 2, 3)
EARLY, LATE = GROUPS[0] + GROUPS[1], GROUPS[2]
PAIRS = tuple((l, l) for l in range(4)) + tuple((l, l + 1) for l in range(3)) + tuple((l + 1, l) for l in range(3))
CHUNK = 1024
SMEM = pl.BlockSpec(memory_space=pltpu.SMEM)
VMEM = pl.BlockSpec(memory_space=pltpu.VMEM)


def permute(x, axis, target):
    size = lax.axis_size(axis)
    return lax.ppermute(x, axis, [(i, target(i) % size) for i in range(size)])


def swap(x, axis, distance=1):
    return permute(x, axis, lambda i: i ^ distance)


def pack_kernel(*refs):
    peers = len(PEERS)
    ids, pieces, outs = refs[:peers], refs[peers:-peers], refs[-peers:]
    for g in range(2):
        for n, (source, target) in enumerate(PAIRS):
            for slots, out in zip(ids, outs):
                tile = slots[g, source] * 3 + (target - source + 1)
                for k, piece in enumerate(pieces):
                    for half in range(2):
                        out[g * len(PAIRS) + n, k, half] = piece[half, tile]


def pack(slots, pieces):
    shape = jax.ShapeDtypeStruct((2 * len(PAIRS), len(pieces), *pieces[0].shape[:1], *pieces[0].shape[2:]), pieces[0].dtype)
    return pl.pallas_call(
        pack_kernel,
        out_shape=[shape] * len(slots),
        in_specs=[SMEM] * len(slots) + [VMEM] * len(pieces),
        out_specs=[VMEM] * len(slots),
        compiler_params=pltpu.CompilerParams(vmem_limit_bytes=8 * 2**20),
        cost_estimate=pl.CostEstimate(flops=1000000, bytes_accessed=2000000, transcendentals=0),
    )(*slots, *pieces)


def tile_of(n, g, slots, counts, pattern):
    source, target = PAIRS[n]
    s, t = slots[g, source], slots[g, target]
    column = target - source + 1
    keep = (t - s == target - source) & (pattern[s, column] == 1) & (max(source, target) < counts[g])
    pair = target // 2
    return s * 3 + column, keep, (pair, source - pair, slice(128 * (target % 2), 128 * (target % 2) + 128))


def place(weights, lead, spot, keep, meta, k, parts):
    pair, row, lanes = spot
    my_xl, my_y, my_q, z = meta[0], meta[1], meta[2], meta[3 + k]
    low, high = my_y % 2 == 1, my_y // 2 == 1
    for half, blocks in enumerate(parts):
        quarter = ((my_xl ^ half) * 2 + z // 4) ^ my_q
        start = pl.multiple_of(row * 512 + quarter * 128 + (z % 4) * 32, 32)
        b = [jnp.where(low, blocks[j ^ 1], blocks[j]) for j in range(4)]
        b = [jnp.where(high, b[j ^ 2], b[j]) for j in range(4)]
        group = jnp.concatenate(b, axis=0)
        weights[(*lead, pair, pl.ds(start, 32), lanes)] = jnp.where(keep, group, jnp.zeros_like(group))


def parts_of(own, recv, tile, index, k):
    by_distance = dict(zip(PEERS, recv))
    return [
        [own[half, tile]] + [by_distance[j][index, k, half] for j in (1, 2, 3)]
        for half in range(2)
    ]


def assemble_kernel(meta, slots, counts, pattern, *refs):
    own, weights = refs[:EARLY], refs[-1]
    recv = (refs[EARLY : EARLY + 3], refs[EARLY + 3 : EARLY + 6])
    for g in range(2):
        weights[g, 0, 1024:, :128] = jnp.zeros((512, 128), weights.dtype)
        weights[g, 1, :512, 128:] = jnp.zeros((512, 128), weights.dtype)
        for n in range(len(PAIRS)):
            tile, keep, spot = tile_of(n, g, slots, counts, pattern)
            for k in range(EARLY):
                part = 0 if k < GROUPS[0] else 1
                parts = parts_of(own[k], recv[part], tile, g * len(PAIRS) + n, k - part * GROUPS[0])
                place(weights, (g,), spot, keep, meta, k, parts)


def assemble(meta, slot_ids, slot_count, pattern, own, recv):
    return pl.pallas_call(
        assemble_kernel,
        out_shape=jax.ShapeDtypeStruct((2, 2, 1536, 256), jnp.bfloat16),
        in_specs=[SMEM] * 4 + [VMEM] * (len(own) + len(recv)),
        out_specs=VMEM,
        compiler_params=pltpu.CompilerParams(vmem_limit_bytes=12 * 2**20),
        cost_estimate=pl.CostEstimate(flops=1000000, bytes_accessed=6000000, transcendentals=0),
    )(meta, slot_ids, slot_count, pattern, *own, *recv)


def rotate_kernel(meta, slots, counts, pattern, staged, *refs):
    own, recv, occupation, quarters = refs[:LATE], refs[LATE : LATE + 3], refs[LATE + 3], refs[LATE + 4 : LATE + 8]
    out, density, weights = refs[LATE + 8 :]
    g, p = pl.program_id(0), pl.program_id(1)

    @pl.when(p == 0)
    def _():
        for pair in range(2):
            weights[pair] = staged[0, pair]
        for n in range(len(PAIRS)):
            tile, keep, spot = tile_of(n, g, slots, counts, pattern)
            for k in range(LATE):
                place(weights, (), spot, keep, meta, EARLY + k, parts_of(own[k], recv, tile, g * len(PAIRS) + n, k))

    total = jnp.zeros((CHUNK, 128), jnp.float32)
    for pair in range(2):
        left = jnp.concatenate([q[0, pair + row] for row in range(3) for q in quarters], axis=1)
        acc = jnp.dot(left, weights[pair], preferred_element_type=jnp.float32)
        rounded = acc.astype(out.dtype)
        for m in range(2):
            mine = rounded[:, 128 * m : 128 * m + 128]
            out[0, 2 * pair + m] = mine
            wide = mine.astype(jnp.float32)
            total = total + wide * wide * occupation[pl.ds(slots[g, 2 * pair + m], 1), :]
    summed = jnp.sum(total.T, axis=0, keepdims=True)
    density[pl.ds(g, 1), pl.ds(pl.multiple_of(p * CHUNK, CHUNK), CHUNK)] = summed


def rotate(meta, slot_ids, slot_count, pattern, staged, own, recv, occupation, quarters):
    blocks, slots_per, points, width = quarters[0].shape
    tile = pl.BlockSpec((1, slots_per, CHUNK, width), lambda g, p: (g, 0, p, 0))
    return pl.pallas_call(
        rotate_kernel,
        grid=(blocks, points // CHUNK),
        out_shape=[
            jax.ShapeDtypeStruct(quarters[0].shape, quarters[0].dtype),
            jax.ShapeDtypeStruct((blocks, points), jnp.float32),
        ],
        in_specs=[SMEM] * 4
        + [pl.BlockSpec((1, *staged.shape[1:]), lambda g, p: (g, 0, 0, 0))]
        + [VMEM] * (len(own) + len(recv) + 1)
        + [tile] * 4,
        out_specs=[tile, pl.BlockSpec((blocks, points), lambda g, p: (0, 0))],
        scratch_shapes=[pltpu.VMEM(staged.shape[1:], jnp.bfloat16)],
        compiler_params=pltpu.CompilerParams(
            dimension_semantics=("arbitrary", "arbitrary"), vmem_limit_bytes=32 * 2**20
        ),
        cost_estimate=pl.CostEstimate(flops=3 * 10**9, bytes_accessed=14 * 10**6, transcendentals=0),
    )(meta, slot_ids, slot_count, pattern, staged, *own, *recv, occupation, *quarters)


def body(orbitals, slot_ids, slot_count, band_tiles, pattern, occupation):
    rows = band_tiles.shape[2]
    z, y = lax.axis_index("z"), lax.axis_index("y")
    odd, second_bit = z % 2, z // 2 % 2
    step = jnp.where(odd == 1, -1, 1)
    z_of = [z, z + step, z - step, z ^ 2, jnp.where(second_bit == 1, z + 2, z - 2), z + 3 * step, z - 3 * step, z + 4]
    meta = jnp.stack(
        [lax.axis_index("xl"), y, lax.axis_index("xh") * 2 + lax.axis_index("c")] + [k & 7 for k in z_of]
    ).astype(jnp.int32)
    tiles = band_tiles.reshape(-1, rows, band_tiles.shape[3])
    here = jnp.stack([tiles, swap(tiles, "xl")])
    far_half = swap(orbitals, "xh")
    near_half = swap(orbitals, "c")
    slots = [swap(slot_ids, "y", k) for k in PEERS]

    def even(i):
        return i ^ 1

    def uneven(i):
        return ((i - 1) ^ 1) + 1

    one = [permute(here, "z", even), permute(here, "z", uneven)]
    two = [swap(here, "z", 2), permute(here, "z", lambda i: ((i - 2) ^ 2) + 2)]
    flag = odd != second_bit
    three = [permute(jnp.where(flag, two[0], two[1]), "z", even), permute(jnp.where(flag, two[1], two[0]), "z", uneven)]
    groups = [[here, *one], two, [*three, swap(two[1], "z", 2)]]
    recv = []
    for blocks in groups:
        packed = pack(slots, blocks)
        recv.append([swap(x, "y", k) for x, k in zip(packed, PEERS)])
    quarters = [orbitals, near_half, far_half, swap(far_half, "c")]
    staged = assemble(meta, slot_ids, slot_count, pattern, groups[0] + groups[1], recv[0] + recv[1])
    rotated, partial = rotate(meta, slot_ids, slot_count, pattern, staged, groups[2], recv[2], occupation, quarters)
    across = swap(partial, "xh")
    diagonal = permute(partial, ("xh", "c"), lambda i: i ^ 3)
    beside = swap(partial, "c")
    return rotated, (partial + beside) + (across + diagonal)


def solution(mesh):
    sizes = (2, 8, 4, 2, 2)
    torus = Mesh(mesh.devices.reshape(sizes), DOM + ORB)
    return jax.shard_map(
        body,
        mesh=torus,
        in_specs=(
            P(DOM, None, None, ORB),
            P(DOM, None),
            P(DOM),
            P(None, None, DOM, ORB),
            P(),
            P(None, ORB),
        ),
        out_specs=(P(DOM, None, None, ORB), P(DOM, None)),
        check_vma=False,
    )
```
